32 devices in a mesh: south: 2 (over core), east: 4 (over z), down: 2 (over x), ens: 2 (over y).
Axes of the slice: x: 2, y: 2, z: 4, core: 2. Of those that a mesh axis runs over, the one named last changes fastest.
Arguments:
- density: float32 [16, 128, 128, 128], P(('ens', 'south'), 'east', 'down'), parts along dimension 0, may hold values from 0.2 to 1.8
- flow_j: float32 [16, 128, 128, 128], P(('ens', 'south'), 'east', 'down'), parts along dimension 0, may hold values from -0.3 to 0.3
- flow_i: float32 [16, 128, 128, 128], P(('ens', 'south'), 'east', 'down'), parts along dimension 0, may hold values from -0.3 to 0.3
- flow_k: float32 [16, 128, 128, 128], P(('ens', 'south'), 'east', 'down'), parts along dimension 0, may hold values from -0.3 to 0.3
Outputs:
- density_end: float32 [16, 128, 128, 128], P(('ens', 'south'), 'east', 'down'), parts along dimension 0
The draws below stay inside these ranges and needn't reach their ends.
There are 2 independent parts, one for each index of `ens`. The reference program is written for one: setup_inputs(seed, part) draws one part's arguments, and reference() takes and returns one part's arrays. A program takes and returns all parts, laid end to end along the dimension named above; each array names one. Nothing has to cross between parts.
All inputs are finite; a program needn't handle non-finite values.
Results may differ from the reference program's by a relative error of at most 0.00002.
Values sent between devices are 32-bit elements; how exact they have to be, the bound alone decides.
A program may use at most 192 MiB of HBM per device.

```python
import jax
import jax.numpy as jnp
from jax import lax

GRID_J = 8
GRID_I = 128
GRID_K = 128
SPECIES = 128
STEPS = 3


def levels(own_key, extent, split, low, top_value):
    def one(axis_at, blocks):
        draws = jax.random.uniform(jax.random.fold_in(jax.random.fold_in(own_key, 6), axis_at), (blocks,), jnp.float32, low / len(split), top_value / len(split))
        return jnp.repeat(jnp.exp(draws), extent[axis_at] // blocks).reshape((-1,) + (1,) * (len(extent) - axis_at - 1))

    gain = one(*split[0])
    for cut in split[1:]:
        gain = gain * one(*cut)
    return gain


def setup_inputs(seed: int = 0, part: int = 0) -> dict:
    keys = jax.random.split(jax.random.key(seed), 5)
    part_keys = jax.random.split(jax.random.fold_in(keys[4], part), 5)
    density = jnp.clip(0.2 + 1.5999999 * jax.random.uniform(part_keys[0], (GRID_J, GRID_I, GRID_K, SPECIES), jnp.float32) ** levels(part_keys[0], (GRID_J, GRID_I, GRID_K, SPECIES), ((0, 2), (1, 4), (2, 2)), -0.2, 0.2), 0.2, 1.8)
    flow_j = jnp.clip(jax.random.uniform(part_keys[1], (GRID_J, GRID_I, GRID_K, SPECIES), jnp.float32, -0.3, 0.3) * levels(part_keys[1], (GRID_J, GRID_I, GRID_K, SPECIES), ((0, 2), (1, 4), (2, 2)), -0.4, 0.0), -0.3, 0.3)
    flow_i = jnp.clip(jax.random.uniform(part_keys[2], (GRID_J, GRID_I, GRID_K, SPECIES), jnp.float32, -0.3, 0.3) * levels(part_keys[2], (GRID_J, GRID_I, GRID_K, SPECIES), ((0, 2), (1, 4), (2, 2)), -0.4, 0.0), -0.3, 0.3)
    flow_k = jnp.clip(jax.random.uniform(part_keys[3], (GRID_J, GRID_I, GRID_K, SPECIES), jnp.float32, -0.3, 0.3) * levels(part_keys[3], (GRID_J, GRID_I, GRID_K, SPECIES), ((0, 2), (1, 4), (2, 2)), -0.4, 0.0), -0.3, 0.3)
    return dict(density=density, flow_j=flow_j, flow_i=flow_i, flow_k=flow_k)


def inner_cells(values, dims):
    for dim in dims:
        values = lax.slice_in_dim(values, 1, values.shape[dim] - 1, axis=dim)
    return values


def side_cells(values, dim, start, dims):
    others = [other for other in dims if other != dim]
    values = inner_cells(values, others)
    return lax.slice_in_dim(values, start, start + values.shape[dim] - 2, axis=dim)


def advance(padded, flow_j, flow_i, flow_k):
    middle = inner_cells(padded, (0, 1, 2))
    lower = [side_cells(padded, dim, 0, (0, 1, 2)) for dim in (0, 1, 2)]
    upper = [side_cells(padded, dim, 2, (0, 1, 2)) for dim in (0, 1, 2)]
    slopes = [above - below for above, below in zip(upper, lower)]
    smooth_rate = 0.05
    spread = lower[0] + upper[0] + lower[1] + upper[1] + lower[2] + upper[2] - 6.0 * middle
    return middle - flow_j * slopes[0] - flow_i * slopes[1] - flow_k * slopes[2] + smooth_rate * spread


def reference(density, flow_j, flow_i, flow_k):
    for step in range(STEPS):
        density = advance(jnp.pad(density, ((1, 1), (1, 1), (1, 1), (0, 0)), mode="constant"), flow_j, flow_i, flow_k)
    return density
```

```python
import functools

import jax
import jax.numpy as jnp
from jax import lax
from jax.experimental import pallas as pl
from jax.experimental.pallas import tpu as pltpu
from jax.sharding import PartitionSpec as P

STEPS = 3
TILE = 8
MESH = pl.DeviceIdType.MESH


def divisor(total, most):
    return max(d for d in range(1, most + 1) if total % d == 0)


def groups(low, high, size):
    return [min(at, high - size) for at in range(low, high, size)]


def kernel(
    counts, density, flow_j, flow_i, flow_k, out,
    field, cj, ci, ck, pack, land,
    load_sem, flow_sem, isend, irecv, ksend, krecv, jsend, jrecv,
):
    nj, ni, nk, lanes = density.shape
    deep = nk + 2 * TILE
    n_south, n_east, n_down = counts
    south, east, down = (lax.axis_index(a) for a in ("south", "east", "down"))
    index = {"south": south, "east": east, "down": down}
    has = {
        ("south", 0): (n_south > 1, south > 0),
        ("south", 1): (n_south > 1, south < n_south - 1),
        ("east", 0): (n_east > 1, east > 0),
        ("east", 1): (n_east > 1, east < n_east - 1),
        ("down", 0): (n_down > 1, down > 0),
        ("down", 1): (n_down > 1, down < n_down - 1),
    }
    inside_k = pl.ds(TILE, nk)
    wide = divisor(ni - 2, 6)
    blocks = (ni - 2) // wide
    cut = 1 + wide * (blocks // 2)
    pieces = [(0, cut), (cut, ni)]

    def neighbour(axis, side):
        return {axis: index[axis] + (1 if side else -1)}

    def when_has(axis, side, act):
        static, dynamic = has[axis, side]
        if static:
            pl.when(dynamic)(act)

    def when_edge(axis, side, act):
        static, dynamic = has[axis, side]
        if static:
            pl.when(jnp.logical_not(dynamic))(act)
        else:
            act()

    first = jnp.where(south == 0, 1, 0) if n_south > 1 else 0

    def plane(t):
        return first * (nj - 1 - t) + (1 - first) * t

    def load(t):
        j, inner = plane(t), pl.ds(1, ni - 2)
        return pltpu.make_async_copy(
            density.at[j, inner], field.at[0, j + 1, pl.ds(2, ni - 2), inside_k], load_sem.at[t]
        )

    def load_face(side):
        i = (ni - 1) * side
        return pltpu.make_async_copy(
            density.at[:, i], field.at[0, pl.ds(1, nj), i + 1, inside_k], load_sem.at[nj + side]
        )

    flows = ((flow_j, cj), (flow_i, ci), (flow_k, ck))

    def load_flow(t, d):
        source, target = flows[d]
        inner = pl.ds(1, ni - 2)
        return pltpu.make_async_copy(
            source.at[plane(t), inner], target.at[plane(t), inner], flow_sem.at[d, t]
        )

    def load_flow_face(side, d):
        source, target = flows[d]
        i = (ni - 1) * side
        return pltpu.make_async_copy(source.at[:, i], target.at[:, i], flow_sem.at[d, nj + side])

    def copy_i(s, side, j):
        return pltpu.make_async_remote_copy(
            src_ref=field.at[s, j + 1, ni if side else 1, inside_k],
            dst_ref=field.at[s, j + 1, 0 if side else ni + 1, inside_k],
            send_sem=isend.at[s, side, j],
            recv_sem=irecv.at[s, 1 - side, j],
            device_id=neighbour("east", side),
            device_id_type=MESH,
        )

    def copy_k(s, side, j):
        return pltpu.make_async_remote_copy(
            src_ref=pack.at[s, side, j],
            dst_ref=land.at[s, 1 - side, j],
            send_sem=ksend.at[s, side, j],
            recv_sem=krecv.at[s, 1 - side, j],
            device_id=neighbour("down", side),
            device_id_type=MESH,
        )

    def copy_j(s, side, piece):
        low, high = pieces[piece]
        rows = pl.ds(low + 1, high - low)
        return pltpu.make_async_remote_copy(
            src_ref=field.at[s, nj if side else 1, rows, inside_k],
            dst_ref=field.at[s, 0 if side else nj + 1, rows, inside_k],
            send_sem=jsend.at[s, side, piece],
            recv_sem=jrecv.at[s, 1 - side, piece],
            device_id=neighbour("south", side),
            device_id_type=MESH,
        )

    def send_i(s, t):
        for side in range(2):
            when_has("east", side, lambda side=side: copy_i(s, side, plane(t)).start())

    def send_k(s, t):
        for side in range(2):
            when_has("down", side, lambda side=side: copy_k(s, side, plane(t)).start())

    def start_j(s, side):
        for piece in range(len(pieces)):
            copy_j(s, side, piece).start()

    def send_j(s, t):
        if n_south > 1 and t == 0:
            pl.when(south == 0)(lambda: start_j(s, 1))
            pl.when(south > 0)(lambda: start_j(s, 0))
        if n_south > 2 and t == nj - 1:
            pl.when((south > 0) & (south < n_south - 1))(lambda: start_j(s, 1))

    waited = set()

    def wait_j(s, t, piece):
        if (s, t, piece) in waited:
            return
        waited.add((s, t, piece))
        if n_south > 1 and t == 0:
            pl.when(south == 0)(lambda: copy_j(s, 0, piece).wait_recv())
            pl.when(south > 0)(lambda: copy_j(s, 1, piece).wait_recv())
        if n_south > 2 and t == nj - 1:
            pl.when((south > 0) & (south < n_south - 1))(
                lambda: copy_j(s, 0, piece).wait_recv()
            )

    def wait_i(s, t):
        for side in range(2):
            when_has("east", side, lambda side=side: copy_i(s, 1 - side, plane(t)).wait_recv())

    def rows(s, j, i, count):
        def at(dj, di, dk):
            return field[s, j + 1 + dj, i + 1 + di, pl.ds(TILE + dk, nk), :]

        line = [at(0, r - 1, 0) for r in range(count + 2)]
        for r in range(count):
            cell = (j, i + r)
            lower = [at(-1, r, 0), line[r], at(0, r, -1)]
            upper = [at(1, r, 0), line[r + 2], at(0, r, 1)]
            gain = [c[cell] for c in (cj, ci, ck)]
            if s == 0:
                gain = [0.05 - g for g in gain]
                for c, g in zip((cj, ci, ck), gain):
                    c[cell] = g
            drift = [g * (u - l) for g, u, l in zip(gain, upper, lower)]
            value = (0.7 * line[r + 1] + 0.1 * (lower[0] + lower[1] + lower[2])) + (
                drift[0] + drift[1] + drift[2]
            )
            if s + 1 < STEPS:
                field[s + 1, j + 1, i + 1 + r, inside_k, :] = value
            else:
                out[cell] = value

    flat = field.reshape(STEPS, nj + 2, (ni + 2) * deep, lanes)
    flat_gain = ck.reshape(nj, ni * nk, lanes)
    flat_out = out.reshape(nj, ni * nk, lanes)

    def edge_field(s, j, i, size, side):
        row = (i + 1) * deep + TILE + (nk - 1) * side
        return flat.at[s, j + 1, pl.ds(row, size, stride=deep), :]

    def edge(ref, j, i, size, side):
        return ref.at[j, pl.ds(i * nk + (nk - 1) * side, size, stride=nk), :]

    def inner(s, t):
        j = plane(t)
        if s == 0:
            for d in range(3):
                load_flow(t, d).wait()
        edges = (t == 0) or (t == nj - 1 and n_south > 2)
        spans = [(0, blocks // 2), (blocks // 2, blocks)] if edges else [(0, blocks)]
        for piece, (low, high) in enumerate(spans):
            if edges:
                wait_j(s, t, piece)

            @pl.loop(low, high)
            def _(b):
                rows(s, j, 1 + b * wide, wide)

    def face(s, t):
        j = plane(t)
        for piece in range(len(pieces)):
            wait_j(s, t, piece)
        for side in range(2):
            def corner(side=side):
                copy_k(s, 1 - side, j).wait_recv()
                row = TILE + nk if side else TILE - 1
                for i in (0, ni - 1):
                    field[s, j + 1, i + 1, pl.ds(row, 1), :] = land[s, side, j, pl.ds(i, 1), :]
            when_has("down", side, corner)
        wait_i(s, t)
        for i in (0, ni - 1):
            rows(s, j, i, 1)
        if s + 1 < STEPS:
            send_i(s + 1, t)

    def fix(s, t):
        j = plane(t)
        for side in range(2):
            def act(side=side):
                parts = []
                for i in groups(1, ni - 1, TILE):
                    gain = edge(flat_gain, j, i, TILE, side)[...]
                    gain = gain if side else 0.1 - gain
                    if s + 1 < STEPS:
                        target = edge_field(s + 1, j, i, TILE, side)
                    else:
                        target = edge(flat_out, j, i, TILE, side)
                    value = target[...] + gain * land[s, side, j, pl.ds(i, TILE), :]
                    parts.append((i, target, value))
                for i, target, value in parts:
                    target[...] = value
                    if s + 1 < STEPS:
                        pack[s + 1, side, j, pl.ds(i, TILE), :] = value
                if s + 1 < STEPS:
                    k = TILE + (nk - 1) * side
                    for i in (0, ni - 1):
                        pack[s + 1, side, j, pl.ds(i, 1), :] = field[
                            s + 1, j + 1, i + 1, pl.ds(k, 1), :
                        ]
            when_has("down", side, act)
        if s + 1 < STEPS:
            send_k(s + 1, t)
            send_j(s + 1, t)

    barrier = pltpu.get_barrier_semaphore()
    for axis, side in has:
        def greet(axis=axis, side=side):
            pl.semaphore_signal(
                barrier, inc=1, device_id=neighbour(axis, side), device_id_type=MESH
            )
        when_has(axis, side, greet)

    for side in range(2):
        load_face(side).start()
    for t in range(nj):
        load(t).start()
    for d in range(3):
        for side in range(2):
            load_flow_face(side, d).start()
    for t in range(nj):
        for d in range(3):
            load_flow(t, d).start()

    zero_row = jnp.zeros((TILE, lanes), jnp.float32)
    zero_line = jnp.zeros((nk, lanes), jnp.float32)
    for s in range(STEPS):
        @pl.loop(0, nj)
        def _(j):
            for i in groups(0, ni, TILE):
                for row in (TILE - 1, TILE + nk):
                    flat[s, j + 1, pl.ds((i + 1) * deep + row, TILE, stride=deep), :] = zero_row

    for side in range(2):
        def zero_j(side=side):
            for s in range(STEPS):
                @pl.loop(0, ni)
                def _(i):
                    field[s, (nj + 1) * side, i + 1, inside_k, :] = zero_line

        def zero_i(side=side):
            for s in range(STEPS):
                @pl.loop(0, nj)
                def _(j):
                    field[s, j + 1, (ni + 1) * side, inside_k, :] = zero_line

        when_edge("south", side, zero_j)
        when_edge("east", side, zero_i)

    pl.semaphore_wait(barrier, sum(jnp.where(d, 1, 0) for s, d in has.values() if s))
    for side in range(2):
        load_face(side).wait()
    for t in range(nj):
        send_i(0, t)
    for t in range(nj):
        load(t).wait()
        for side in range(2):
            def first_pack(side=side):
                for i in groups(0, ni, TILE):
                    pack[0, side, plane(t), pl.ds(i, TILE), :] = edge_field(
                        0, plane(t), i, TILE, side
                    )[...]
            when_has("down", side, first_pack)
        send_k(0, t)
        send_j(0, t)
    for d in range(3):
        for side in range(2):
            load_flow_face(side, d).wait()

    inner(0, 0)
    for t in range(nj):
        if t < 2:
            face(0, t)
            fix(0, t)
            if t + 1 < min(nj, 2):
                inner(0, t + 1)
        else:
            face(0, t)
            inner(0, t)
            fix(0, t)
    inner(1, 1)
    inner(1, 0)
    for s in range(1, STEPS):
        for t in range(nj):
            face(s, t)
            fix(s, t)
            if t + 2 < nj:
                inner(s, t + 2)
            elif s + 1 < STEPS:
                if t == nj - 2 and nj > 3:
                    inner(s + 1, 1)
                if t == nj - 1:
                    if nj <= 3:
                        inner(s + 1, 1)
                    inner(s + 1, 0)

    for s in range(STEPS):
        for side in range(2):
            for piece in range(len(pieces)):
                when_has(
                    "south", side, lambda side=side, piece=piece: copy_j(s, side, piece).wait_send()
                )
            for j in range(nj):
                when_has("east", side, lambda side=side, j=j: copy_i(s, side, j).wait_send())
                when_has("down", side, lambda side=side, j=j: copy_k(s, side, j).wait_send())


def per_device(counts, density, flow_j, flow_i, flow_k):
    nj, ni, nk, lanes = density.shape
    f32 = jnp.float32
    dma = pltpu.SemaphoreType.DMA
    return pl.pallas_call(
        functools.partial(kernel, counts),
        out_shape=pltpu.VMEM(density.shape, f32),
        in_specs=[pl.BlockSpec(memory_space=pl.ANY)] * 4,
        out_specs=pl.BlockSpec(memory_space=pltpu.VMEM),
        scratch_shapes=[
            pltpu.VMEM((STEPS, nj + 2, ni + 2, nk + 2 * TILE, lanes), f32),
            pltpu.VMEM((nj, ni, nk, lanes), f32),
            pltpu.VMEM((nj, ni, nk, lanes), f32),
            pltpu.VMEM((nj, ni, nk, lanes), f32),
            pltpu.VMEM((STEPS, 2, nj, ni, lanes), f32),
            pltpu.VMEM((STEPS, 2, nj, ni, lanes), f32),
            dma((nj + 2,)),
            dma((3, nj + 2)),
            dma((STEPS, 2, nj)),
            dma((STEPS, 2, nj)),
            dma((STEPS, 2, nj)),
            dma((STEPS, 2, nj)),
            dma((STEPS, 2, 2)),
            dma((STEPS, 2, 2)),
        ],
        compiler_params=pltpu.CompilerParams(
            collective_id=0, has_side_effects=True, vmem_limit_bytes=58 * 1024 * 1024
        ),
    )(density, flow_j, flow_i, flow_k)


def solution(mesh):
    spec = P(("ens", "south"), "east", "down", None)
    counts = tuple(mesh.shape[a] for a in ("south", "east", "down"))
    return jax.shard_map(
        functools.partial(per_device, counts),
        mesh=mesh,
        in_specs=(spec,) * 4,
        out_specs=spec,
        check_vma=False,
    )
```

```python
import functools

import jax
import jax.numpy as jnp
from jax import lax
from jax.experimental import pallas as pl
from jax.experimental.pallas import tpu as pltpu
from jax.sharding import PartitionSpec as P

STEPS = 3
TILE = 8
MESH = pl.DeviceIdType.MESH
PLAN = """
L010 L011 L000 L001 F000 F010 F001 F011 K00 Z10 Z11
L020 F020 F021 K01 Z12 L021 F030 F031 K02 Z13 L030 F040 F041 Z14 L031 K03
L110 L111 S0 F100 F101 F110 F111 L100 L101 K10 Z20 Z21
F120 F121 K11 L120 Z22 L121 F130 F131 K12 Z23 L130 F140 F141 Z24 L131 K13
L210 L211 L220 L221 L230 L231 L200 L201 S1
F200 F201 F210 F211 K20 F220 F221 K21 F230 F231 K22 S2 F240 F241 K23
"""


def divisor(total, most):
    return max(d for d in range(1, most + 1) if total % d == 0)


def groups(low, high, size):
    return [min(at, high - size) for at in range(low, high, size)]


def kernel(
    counts, density, flow_j, flow_i, flow_k, out,
    field, cj, ci, ck, pack, land,
    load_sem, flow_sem, isend, irecv, ksend, krecv, jsend, jrecv,
):
    nj, ni, nk, lanes = density.shape
    deep = nk + 2 * TILE
    n_south, n_east, n_down = counts
    south, east, down = (lax.axis_index(a) for a in ("south", "east", "down"))
    index = {"south": south, "east": east, "down": down}
    has = {
        ("south", 0): (n_south > 1, south > 0),
        ("south", 1): (n_south > 1, south < n_south - 1),
        ("east", 0): (n_east > 1, east > 0),
        ("east", 1): (n_east > 1, east < n_east - 1),
        ("down", 0): (n_down > 1, down > 0),
        ("down", 1): (n_down > 1, down < n_down - 1),
    }
    inside_k = pl.ds(TILE, nk)
    wide = divisor(ni - 2, 6)
    blocks = (ni - 2) // wide
    cut = 1 + wide * (blocks // 2)
    pieces = [(0, cut), (cut, ni)]
    half = max(TILE, nk // 2 // TILE * TILE)
    chunks = [(0, 0, half), (0, half, nk - half)] + [(t, 0, nk) for t in range(1, nj)]

    def neighbour(axis, side):
        return {axis: index[axis] + (1 if side else -1)}

    def when_has(axis, side, act):
        static, dynamic = has[axis, side]
        if static:
            pl.when(dynamic)(act)

    def when_edge(axis, side, act):
        static, dynamic = has[axis, side]
        if static:
            pl.when(jnp.logical_not(dynamic))(act)
        else:
            act()

    first = jnp.where(south == 0, 1, 0) if n_south > 1 else 0

    def plane(t):
        return first * (nj - 1 - t) + (1 - first) * t

    between = pl.ds(1, ni - 2)

    def load(t):
        return pltpu.make_async_copy(
            density.at[plane(t), between],
            field.at[0, plane(t) + 1, pl.ds(2, ni - 2), inside_k],
            load_sem.at[t],
        )

    def load_face(low, rows, high):
        return pltpu.make_async_copy(
            density.at[:, pl.ds(low, rows)],
            field.at[0, pl.ds(1, nj), pl.ds(high, rows), inside_k],
            load_sem.at[nj],
        )

    flows = ((flow_j, cj), (flow_i, ci), (flow_k, ck))

    def load_flow(t, source, target):
        return pltpu.make_async_copy(
            source.at[plane(t), between], target.at[plane(t), between], flow_sem.at[t]
        )

    def load_flow_face(low, rows, source, target):
        return pltpu.make_async_copy(
            source.at[:, pl.ds(low, rows)], target.at[:, pl.ds(low, rows)], flow_sem.at[nj]
        )

    def copy_i(s, side, c):
        t, k, size = chunks[c]
        j, part = plane(t), pl.ds(TILE + k, size)
        return pltpu.make_async_remote_copy(
            src_ref=field.at[s, j + 1, ni if side else 1, part],
            dst_ref=field.at[s, j + 1, 0 if side else ni + 1, part],
            send_sem=isend.at[s % 2, side],
            recv_sem=irecv.at[s % 2, 1 - side, c],
            device_id=neighbour("east", side),
            device_id_type=MESH,
        )

    def copy_k(s, side, j):
        return pltpu.make_async_remote_copy(
            src_ref=pack.at[s, side, j],
            dst_ref=land.at[s, 1 - side, j],
            send_sem=ksend.at[s % 2, side],
            recv_sem=krecv.at[s % 2, 1 - side, j],
            device_id=neighbour("down", side),
            device_id_type=MESH,
        )

    def copy_j(s, side, piece):
        low, high = pieces[piece]
        rows = pl.ds(low + 1, high - low)
        return pltpu.make_async_remote_copy(
            src_ref=field.at[s, nj if side else 1, rows, inside_k],
            dst_ref=field.at[s, 0 if side else nj + 1, rows, inside_k],
            send_sem=jsend.at[s % 2, side],
            recv_sem=jrecv.at[s % 2, 1 - side, piece],
            device_id=neighbour("south", side),
            device_id_type=MESH,
        )

    def send_i(s, c, side, late):
        static, dynamic = has["east", side]
        if static and n_south > 1:
            pl.when(dynamic & ((south > 0) if late else (south == 0)))(copy_i(s, side, c).start)
        elif static and not late:
            pl.when(dynamic)(copy_i(s, side, c).start)

    def send_late(s, c):
        for side in range(2):
            send_i(s, c, side, True)

    def send_k(s, t):
        for side in range(2):
            when_has("down", side, lambda side=side: copy_k(s, side, plane(t)).start())

    def start_j(s, side):
        for piece in range(len(pieces)):
            copy_j(s, side, piece).start()

    def send_j(s, t):
        if n_south > 1 and t == 0:
            pl.when(south == 0)(lambda: start_j(s, 1))
            pl.when(south > 0)(lambda: start_j(s, 0))
        if n_south > 2 and t == nj - 1:
            pl.when((south > 0) & (south < n_south - 1))(lambda: start_j(s, 1))

    waited = set()

    def wait_j(s, t, piece):
        if (s, t, piece) in waited:
            return
        waited.add((s, t, piece))
        if n_south > 1 and t == 0:
            pl.when(south == 0)(lambda: copy_j(s, 0, piece).wait_recv())
            pl.when(south > 0)(lambda: copy_j(s, 1, piece).wait_recv())
        if n_south > 2 and t == nj - 1:
            pl.when((south > 0) & (south < n_south - 1))(
                lambda: copy_j(s, 0, piece).wait_recv()
            )

    def wait_i(s, c, side):
        when_has("east", side, lambda: copy_i(s, 1 - side, c).wait_recv())

    def rows(s, j, i, count, k=0, size=nk):
        def at(dj, di, dk):
            return field[s, j + 1 + dj, i + 1 + di, pl.ds(TILE + k + dk, size), :]

        line = [at(0, r - 1, 0) for r in range(count + 2)]
        for r in range(count):
            cell = (j, i + r, pl.ds(k, size))
            lower = [at(-1, r, 0), line[r], at(0, r, -1)]
            upper = [at(1, r, 0), line[r + 2], at(0, r, 1)]
            gain = [c[cell] for c in (cj, ci, ck)]
            if s == 0:
                gain = [0.05 - g for g in gain]
                for c, g in zip((cj, ci, ck), gain):
                    c[cell] = g
            drift = [g * (u - l) for g, u, l in zip(gain, upper, lower)]
            value = (0.7 * line[r + 1] + 0.1 * (lower[0] + lower[1] + lower[2])) + (
                drift[0] + drift[1] + drift[2]
            )
            if s + 1 < STEPS:
                field[s + 1, j + 1, i + 1 + r, pl.ds(TILE + k, size), :] = value
            else:
                out[cell] = value

    flat = field.reshape(STEPS, nj + 2, (ni + 2) * deep, lanes)
    flat_gain = ck.reshape(nj, ni * nk, lanes)
    flat_out = out.reshape(nj, ni * nk, lanes)

    def edge_field(s, j, i, size, side):
        row = (i + 1) * deep + TILE + (nk - 1) * side
        return flat.at[s, j + 1, pl.ds(row, size, stride=deep), :]

    def edge(ref, j, i, size, side):
        return ref.at[j, pl.ds(i * nk + (nk - 1) * side, size, stride=nk), :]

    def start_flow(t):
        for flow in flows:
            load_flow(t, *flow).start()

    def wait_flow(t):
        pltpu.make_async_copy(
            flow_j.at[pl.ds(0, 3), between], cj.at[pl.ds(0, 3), between], flow_sem.at[t]
        ).wait()
        for later in [2] if t == 1 else range(3, nj) if t == 0 else []:
            start_flow(later)

    def inner(s, t, part):
        if s == 0 and (t, "flow") not in waited:
            waited.add((t, "flow"))
            wait_flow(t)
        edges = (t == 0) or (t == nj - 1 and n_south > 2)
        low, high = [(0, blocks // 2), (blocks // 2, blocks)][part]
        if edges:
            wait_j(s, t, part)

        @pl.loop(low, high)
        def _(b):
            rows(s, plane(t), 1 + b * wide, wide)

    def wait_k(s, t):
        if (s, t, "k") in waited:
            return
        waited.add((s, t, "k"))
        j = plane(t)
        for side in range(2):
            def corner(side=side):
                copy_k(s, 1 - side, j).wait_recv()
                row = TILE + nk if side else TILE - 1
                for i in (0, ni - 1):
                    field[s, j + 1, i + 1, pl.ds(row, 1), :] = land[s, side, j, pl.ds(i, 1), :]
            when_has("down", side, corner)

    def face(s, c, side):
        t, k, size = chunks[c]
        for piece in range(len(pieces)):
            wait_j(s, t, piece)
        wait_k(s, t)
        wait_i(s, c, side)
        rows(s, plane(t), (ni - 1) * side, 1, k, size)
        if s + 1 < STEPS:
            send_i(s + 1, c, side, False)

    def fix(s, t):
        j = plane(t)
        for side in range(2):
            def act(side=side):
                parts = []
                for i in groups(1, ni - 1, TILE):
                    gain = edge(flat_gain, j, i, TILE, side)[...]
                    gain = gain if side else 0.1 - gain
                    if s + 1 < STEPS:
                        target = edge_field(s + 1, j, i, TILE, side)
                    else:
                        target = edge(flat_out, j, i, TILE, side)
                    value = target[...] + gain * land[s, side, j, pl.ds(i, TILE), :]
                    parts.append((i, target, value))
                for i, target, value in parts:
                    target[...] = value
                    if s + 1 < STEPS:
                        pack[s + 1, side, j, pl.ds(i, TILE), :] = value
                if s + 1 < STEPS:
                    k = TILE + (nk - 1) * side
                    for i in (0, ni - 1):
                        pack[s + 1, side, j, pl.ds(i, 1), :] = field[
                            s + 1, j + 1, i + 1, pl.ds(k, 1), :
                        ]
            when_has("down", side, act)
        if s + 1 < STEPS:
            send_k(s + 1, t)
            send_j(s + 1, t)

    def drain(s):
        for side in range(2):
            def sent(side=side):
                pltpu.make_async_remote_copy(
                    src_ref=field.at[s, pl.ds(1, nj), ni if side else 1, inside_k],
                    dst_ref=field.at[s, pl.ds(1, nj), 0 if side else ni + 1, inside_k],
                    send_sem=isend.at[s % 2, side],
                    recv_sem=irecv.at[s % 2, 1 - side, 0],
                    device_id=neighbour("east", side),
                    device_id_type=MESH,
                ).wait_send()
            when_has("east", side, sent)

            def sent(side=side):
                pltpu.make_async_remote_copy(
                    src_ref=pack.at[s, side],
                    dst_ref=land.at[s, 1 - side],
                    send_sem=ksend.at[s % 2, side],
                    recv_sem=krecv.at[s % 2, 1 - side, 0],
                    device_id=neighbour("down", side),
                    device_id_type=MESH,
                ).wait_send()
            when_has("down", side, sent)

            def sent(side=side):
                rows = pl.ds(1, ni)
                pltpu.make_async_remote_copy(
                    src_ref=field.at[s, nj if side else 1, rows, inside_k],
                    dst_ref=field.at[s, 0 if side else nj + 1, rows, inside_k],
                    send_sem=jsend.at[s % 2, side],
                    recv_sem=jrecv.at[s % 2, 1 - side, 0],
                    device_id=neighbour("south", side),
                    device_id_type=MESH,
                ).wait_send()
            when_has("south", side, sent)

    def wait_load(t):
        load(t).wait()

    def pack_first(t):
        for side in range(2):
            def act(side=side):
                for i in groups(0, ni, TILE):
                    pack[0, side, plane(t), pl.ds(i, TILE), :] = edge_field(
                        0, plane(t), i, TILE, side
                    )[...]
            when_has("down", side, act)

    def wait_barrier():
        pl.semaphore_wait(barrier, sum(jnp.where(d, 1, 0) for s, d in has.values() if s))

    def wait_face():
        load_face(0, 2, 1).wait()

    def wait_flow_face():
        load_flow_face(0, 6, flow_j, cj).wait()

    barrier = pltpu.get_barrier_semaphore()
    for axis, side in has:
        def greet(axis=axis, side=side):
            pl.semaphore_signal(
                barrier, inc=1, device_id=neighbour(axis, side), device_id_type=MESH
            )
        when_has(axis, side, greet)

    for low in (0, ni - 1):
        load_face(low, 1, low + 1).start()
    for t in range(nj):
        load(t).start()

    def clear():
        zero_row = jnp.zeros((TILE, lanes), jnp.float32)
        zero_line = jnp.zeros((nk, lanes), jnp.float32)
        for s in range(STEPS):
            @pl.loop(0, nj)
            def _(j):
                for i in groups(0, ni, TILE):
                    for row in (TILE - 1, TILE + nk):
                        flat[s, j + 1, pl.ds((i + 1) * deep + row, TILE, stride=deep), :] = zero_row

        for side in range(2):
            def zero_j(side=side):
                for s in range(STEPS):
                    @pl.loop(0, ni)
                    def _(i):
                        field[s, (nj + 1) * side, i + 1, inside_k, :] = zero_line

            def zero_i(side=side):
                for s in range(STEPS):
                    @pl.loop(0, nj)
                    def _(j):
                        field[s, j + 1, (ni + 1) * side, inside_k, :] = zero_line

            when_edge("south", side, zero_j)
            when_edge("east", side, zero_i)

    clear()
    for flow in flows:
        for low in (0, ni - 1):
            load_flow_face(low, 1, *flow).start()
    start_flow(1)
    wait_barrier()
    wait_face()
    for c in range(len(chunks)):
        for side in range(2):
            send_i(0, c, side, False)
    start_flow(0)
    for t in range(nj):
        if t == 2:
            for c in range(len(chunks)):
                send_late(0, c)
        wait_load(t)
        pack_first(t)
        send_k(0, t)
        send_j(0, t)
    wait_flow_face()

    def order():
        if nj == 4:
            for word in PLAN.split():
                yield word[0], *map(int, word[1:])
            return
        for s in range(STEPS):
            for t in [*range(1, nj), 0]:
                for part in range(2):
                    yield "L", s, t, part
            yield "S", s
            for c, (t, k, size) in enumerate(chunks):
                for side in range(2):
                    yield "F", s, c, side
                if s + 1 < STEPS:
                    yield "Z", s + 1, c
                if k + size == nk:
                    yield "K", s, t

    acts = {"L": inner, "F": face, "K": fix, "S": drain, "Z": send_late}
    for name, *where in order():
        acts[name](*where)


def per_device(counts, density, flow_j, flow_i, flow_k):
    nj, ni, nk, lanes = density.shape
    f32 = jnp.float32
    dma = pltpu.SemaphoreType.DMA
    return pl.pallas_call(
        functools.partial(kernel, counts),
        out_shape=pltpu.VMEM(density.shape, f32),
        in_specs=[pl.BlockSpec(memory_space=pl.ANY)] * 4,
        out_specs=pl.BlockSpec(memory_space=pltpu.VMEM),
        scratch_shapes=[
            pltpu.VMEM((STEPS, nj + 2, ni + 2, nk + 2 * TILE, lanes), f32),
            pltpu.VMEM((nj, ni, nk, lanes), f32),
            pltpu.VMEM((nj, ni, nk, lanes), f32),
            pltpu.VMEM((nj, ni, nk, lanes), f32),
            pltpu.VMEM((STEPS, 2, nj, ni, lanes), f32),
            pltpu.VMEM((STEPS, 2, nj, ni, lanes), f32),
            dma((nj + 1,)),
            dma((nj + 1,)),
            dma((2, 2)),
            dma((2, 2, nj + 1)),
            dma((2, 2)),
            dma((2, 2, nj)),
            dma((2, 2)),
            dma((2, 2, 2)),
        ],
        compiler_params=pltpu.CompilerParams(
            collective_id=0, has_side_effects=True, vmem_limit_bytes=58 * 1024 * 1024
        ),
    )(density, flow_j, flow_i, flow_k)


def solution(mesh):
    spec = P(("ens", "south"), "east", "down", None)
    counts = tuple(mesh.shape[a] for a in ("south", "east", "down"))
    return jax.shard_map(
        functools.partial(per_device, counts),
        mesh=mesh,
        in_specs=(spec,) * 4,
        out_specs=spec,
        check_vma=False,
    )
```

```python
import functools

import jax
import jax.numpy as jnp
from jax import lax
from jax.experimental import pallas as pl
from jax.experimental.pallas import tpu as pltpu
from jax.sharding import PartitionSpec as P

STEPS = 3
TILE = 8
MESH = pl.DeviceIdType.MESH
PLAN = (
    "E01", "M01", "P1", "F000", "F010", "P0", "F001", "F011", "K00", "J1", "Z10", "Z11",
    "E02", "F020", "F021", "K01", "Z12", "F030", "F040", "F031", "K02", "Z13", "E03", "F041",
    "K03", "Z14", "M02", "M03", "X1", "E11", "D0", "F100", "F110", "F101", "F111", "E10",
    "K10", "Z20", "Z21", "M10", "J2", "F120", "F121", "K11", "Z22", "E12", "M11", "F130",
    "E13", "F140", "F131", "K12", "Z23", "F141", "K13", "Z24", "M12", "M13", "X2", "E21",
    "M21", "E22", "M22", "E23", "M23", "E20", "M20", "D1", "F200", "F201", "F210", "F211",
    "K20", "F220", "F221", "K21", "F230", "F231", "K22", "F240", "K23", "D2", "F241",
)


def divisor(total, most):
    return max(d for d in range(1, most + 1) if total % d == 0)


def groups(low, high, size):
    return [min(at, high - size) for at in range(low, high, size)]


def kernel(
    counts, density, flow_j, flow_i, flow_k, out,
    field, cj, ci, ck, pack, land,
    load_sem, flow_sem, isend, irecv, ksend, krecv, jsend, jrecv,
):
    nj, ni, nk, lanes = density.shape
    deep = nk + 2 * TILE
    n_south, n_east, n_down = counts
    south, east, down = (lax.axis_index(a) for a in ("south", "east", "down"))
    index = {"south": south, "east": east, "down": down}
    has = {
        ("south", 0): (n_south > 1, south > 0),
        ("south", 1): (n_south > 1, south < n_south - 1),
        ("east", 0): (n_east > 1, east > 0),
        ("east", 1): (n_east > 1, east < n_east - 1),
        ("down", 0): (n_down > 1, down > 0),
        ("down", 1): (n_down > 1, down < n_down - 1),
    }
    inside_k = pl.ds(TILE, nk)
    wide = divisor(ni - 2, 10)
    tall = divisor(ni - 2, 30)
    pieces = [(0, ni // 2), (ni // 2, ni)]
    half = max(TILE, nk // 2 // TILE * TILE)
    chunks = [(0, 0, half), (0, half, nk - half)] + [(t, 0, nk) for t in range(1, nj)]

    def slot(axis, side):
        return side if counts[("south", "east", "down").index(axis)] > 2 else 0

    def neighbour(axis, side):
        return {axis: index[axis] + (1 if side else -1)}

    def when_has(axis, side, act):
        static, dynamic = has[axis, side]
        if static:
            pl.when(dynamic)(act)

    def when_edge(axis, side, act):
        static, dynamic = has[axis, side]
        if static:
            pl.when(jnp.logical_not(dynamic))(act)
        else:
            act()

    first = jnp.where(south == 0, 1, 0) if n_south > 1 else 0

    def plane(t):
        return first * (nj - 1 - t) + (1 - first) * t

    between = pl.ds(1, ni - 2)

    def load(t):
        return pltpu.make_async_copy(
            density.at[plane(t), between],
            field.at[0, plane(t) + 1, pl.ds(2, ni - 2), inside_k],
            load_sem.at[t],
        )

    def load_face(low, rows, high):
        return pltpu.make_async_copy(
            density.at[:, pl.ds(low, rows)],
            field.at[0, pl.ds(1, nj), pl.ds(high, rows), inside_k],
            load_sem.at[nj],
        )

    flows = ((flow_j, cj), (flow_i, ci), (flow_k, ck))

    def flow_slot(t):
        return flow_sem.at[t] if t < 2 else load_sem.at[t - 2]

    def load_flow(t, source, target):
        return pltpu.make_async_copy(
            source.at[plane(t), between], target.at[plane(t), between], flow_slot(t)
        )

    def load_flow_face(low, rows, source, target):
        return pltpu.make_async_copy(
            source.at[:, pl.ds(low, rows)], target.at[:, pl.ds(low, rows)], flow_sem.at[2]
        )

    def copy_i(s, side, c):
        t, k, size = chunks[c]
        j, part = plane(t), pl.ds(TILE + k, size)
        return pltpu.make_async_remote_copy(
            src_ref=field.at[s, j + 1, ni if side else 1, part],
            dst_ref=field.at[s, j + 1, 0 if side else ni + 1, part],
            send_sem=isend.at[s % 2, side],
            recv_sem=irecv.at[s % 2, 1 - side, c],
            device_id=neighbour("east", side),
            device_id_type=MESH,
        )

    def copy_k(s, side, j):
        return pltpu.make_async_remote_copy(
            src_ref=pack.at[s, side, j],
            dst_ref=land.at[s, 1 - side, j],
            send_sem=ksend.at[s % 2, slot("down", side)],
            recv_sem=krecv.at[s % 2, slot("down", 1 - side), j],
            device_id=neighbour("down", side),
            device_id_type=MESH,
        )

    def copy_j(s, side, piece):
        low, high = pieces[piece]
        rows = pl.ds(low + 1, high - low)
        return pltpu.make_async_remote_copy(
            src_ref=field.at[s, nj if side else 1, rows, inside_k],
            dst_ref=field.at[s, 0 if side else nj + 1, rows, inside_k],
            send_sem=jsend.at[slot("south", side)],
            recv_sem=jrecv.at[s % 2, slot("south", 1 - side), piece],
            device_id=neighbour("south", side),
            device_id_type=MESH,
        )

    def send_i(s, c, side, late):
        static, dynamic = has["east", side]
        if static and n_south > 1:
            pl.when(dynamic & ((south > 0) if late else (south == 0)))(copy_i(s, side, c).start)
        elif static and not late:
            pl.when(dynamic)(copy_i(s, side, c).start)

    def send_late(s, c):
        for side in range(2):
            send_i(s, c, side, True)

    def send_k(s, t):
        for side in range(2):
            when_has("down", side, lambda side=side: copy_k(s, side, plane(t)).start())

    def start_j(s, side):
        for piece in range(len(pieces)):
            copy_j(s, side, piece).start()

    def send_j(s):
        if n_south > 1:
            pl.when(south == 0)(lambda: start_j(s, 1))
            pl.when(south > 0)(lambda: start_j(s, 0))

    def send_far_j(s):
        if n_south > 2:
            pl.when((south > 0) & (south < n_south - 1))(lambda: start_j(s, 1))

    waited = set()

    def wait_j(s, t, piece):
        if (s, t, piece) in waited:
            return
        waited.add((s, t, piece))
        if n_south > 1 and t == 0:
            pl.when(south == 0)(lambda: copy_j(s, 0, piece).wait_recv())
            pl.when(south > 0)(lambda: copy_j(s, 1, piece).wait_recv())
        if n_south > 2 and t == nj - 1:
            pl.when((south > 0) & (south < n_south - 1))(
                lambda: copy_j(s, 0, piece).wait_recv()
            )

    def wait_i(s, c, side):
        when_has("east", side, lambda: copy_i(s, 1 - side, c).wait_recv())

    def rows(s, j, i, count, k=0, size=nk):
        def at(dj, di, dk):
            return field[s, j + 1 + dj, i + 1 + di, pl.ds(TILE + k + dk, size), :]

        line = [at(0, r - 1, 0) for r in range(count + 2)]
        for r in range(count):
            cell = (j, i + r, pl.ds(k, size))
            lower = [at(-1, r, 0), line[r], at(0, r, -1)]
            upper = [at(1, r, 0), line[r + 2], at(0, r, 1)]
            gain = [c[cell] for c in (cj, ci, ck)]
            if s == 0:
                gain = [0.05 - g for g in gain]
                for c, g in zip((cj, ci, ck), gain):
                    c[cell] = g
            drift = [g * (u - l) for g, u, l in zip(gain, upper, lower)]
            value = (0.7 * line[r + 1] + 0.1 * (lower[0] + lower[1] + lower[2])) + (
                drift[0] + drift[1] + drift[2]
            )
            if s + 1 < STEPS:
                field[s + 1, j + 1, i + 1 + r, pl.ds(TILE + k, size), :] = value
            else:
                out[cell] = value

    flat = field.reshape(STEPS, nj + 2, (ni + 2) * deep, lanes)
    flat_gain = ck.reshape(nj, ni * nk, lanes)
    flat_out = out.reshape(nj, ni * nk, lanes)

    def edge_field(s, j, i, size, side):
        row = (i + 1) * deep + TILE + (nk - 1) * side
        return flat.at[s, j + 1, pl.ds(row, size, stride=deep), :]

    def edge(ref, j, i, size, side):
        return ref.at[j, pl.ds(i * nk + (nk - 1) * side, size, stride=nk), :]

    def start_flow(t):
        for flow in flows:
            load_flow(t, *flow).start()

    def wait_flow(t):
        pltpu.make_async_copy(
            flow_j.at[pl.ds(0, 3), between], cj.at[pl.ds(0, 3), between], flow_slot(t)
        ).wait()
        for later in [2] if t == 1 else range(3, nj) if t == 0 else []:
            start_flow(later)

    def ready(s, t):
        if s == 0 and (t, "flow") not in waited:
            waited.add((t, "flow"))
            wait_flow(t)
        for piece in range(len(pieces)):
            wait_j(s, t, piece)

    def edge_tiles(s, t):
        ready(s, t)

        @pl.loop(0, (ni - 2) // tall)
        def _(b):
            for k in sorted({0, nk - TILE}):
                rows(s, plane(t), 1 + b * tall, tall, k, TILE)

    def middle(s, t):
        ready(s, t)
        if nk > 2 * TILE:
            @pl.loop(0, (ni - 2) // wide)
            def _(b):
                rows(s, plane(t), 1 + b * wide, wide, TILE, nk - 2 * TILE)

    def wait_k(s, t):
        if (s, t, "k") in waited:
            return
        waited.add((s, t, "k"))
        j = plane(t)
        for side in range(2):
            def corner(side=side):
                copy_k(s, 1 - side, j).wait_recv()
                row = TILE + nk if side else TILE - 1
                for i in (0, ni - 1):
                    field[s, j + 1, i + 1, pl.ds(row, 1), :] = land[s, side, j, pl.ds(i, 1), :]
            when_has("down", side, corner)

    def face(s, c, side):
        t, k, size = chunks[c]
        for piece in range(len(pieces)):
            wait_j(s, t, piece)
        wait_k(s, t)
        if s == 0 and "faces" not in waited:
            waited.add("faces")
            wait_flow_face()
        wait_i(s, c, side)
        rows(s, plane(t), (ni - 1) * side, 1, k, size)
        if s + 1 < STEPS:
            send_i(s + 1, c, side, False)

    def fix(s, t):
        j = plane(t)
        for side in range(2):
            def act(side=side):
                parts = []
                for i in groups(1, ni - 1, TILE):
                    gain = edge(flat_gain, j, i, TILE, side)[...]
                    gain = gain if side else 0.1 - gain
                    if s + 1 < STEPS:
                        target = edge_field(s + 1, j, i, TILE, side)
                    else:
                        target = edge(flat_out, j, i, TILE, side)
                    value = target[...] + gain * land[s, side, j, pl.ds(i, TILE), :]
                    parts.append((i, target, value))
                for i, target, value in parts:
                    target[...] = value
                    if s + 1 < STEPS:
                        pack[s + 1, side, j, pl.ds(i, TILE), :] = value
                if s + 1 < STEPS:
                    k = TILE + (nk - 1) * side
                    for i in (0, ni - 1):
                        pack[s + 1, side, j, pl.ds(i, 1), :] = field[
                            s + 1, j + 1, i + 1, pl.ds(k, 1), :
                        ]
            when_has("down", side, act)
        if s + 1 < STEPS:
            send_k(s + 1, t)

    def drain_i(s):
        for side in range(2):
            def sent(side=side):
                pltpu.make_async_remote_copy(
                    src_ref=field.at[s, pl.ds(1, nj), ni if side else 1, inside_k],
                    dst_ref=field.at[s, pl.ds(1, nj), 0 if side else ni + 1, inside_k],
                    send_sem=isend.at[s % 2, side],
                    recv_sem=irecv.at[s % 2, 1 - side, 0],
                    device_id=neighbour("east", side),
                    device_id_type=MESH,
                ).wait_send()
            when_has("east", side, sent)

    def drain_k(s):
        for side in range(2):
            def sent(side=side):
                pltpu.make_async_remote_copy(
                    src_ref=pack.at[s, side],
                    dst_ref=land.at[s, 1 - side],
                    send_sem=ksend.at[s % 2, slot("down", side)],
                    recv_sem=krecv.at[s % 2, slot("down", 1 - side), 0],
                    device_id=neighbour("down", side),
                    device_id_type=MESH,
                ).wait_send()
            when_has("down", side, sent)

    def drain_j(s):
        for side in range(2):
            def sent(side=side):
                rows = pl.ds(1, ni)
                pltpu.make_async_remote_copy(
                    src_ref=field.at[s, nj if side else 1, rows, inside_k],
                    dst_ref=field.at[s, 0 if side else nj + 1, rows, inside_k],
                    send_sem=jsend.at[slot("south", side)],
                    recv_sem=jrecv.at[s % 2, slot("south", 1 - side), 0],
                    device_id=neighbour("south", side),
                    device_id_type=MESH,
                ).wait_send()
            when_has("south", side, sent)

    def drain(s):
        drain_i(s)
        drain_k(s)

    def wait_load(t):
        load(t).wait()

    def pack_first(t):
        for side in range(2):
            def act(side=side):
                for i in groups(0, ni, TILE):
                    pack[0, side, plane(t), pl.ds(i, TILE), :] = edge_field(
                        0, plane(t), i, TILE, side
                    )[...]
            when_has("down", side, act)

    def wait_barrier():
        pl.semaphore_wait(barrier, sum(jnp.where(d, 1, 0) for s, d in has.values() if s))

    def wait_face():
        load_face(0, 2, 1).wait()

    def wait_flow_face():
        load_flow_face(0, 6, flow_j, cj).wait()

    barrier = pltpu.get_barrier_semaphore()
    for axis, side in has:
        def greet(axis=axis, side=side):
            pl.semaphore_signal(
                barrier, inc=1, device_id=neighbour(axis, side), device_id_type=MESH
            )
        when_has(axis, side, greet)

    for low in (0, ni - 1):
        load_face(low, 1, low + 1).start()
    for t in range(nj):
        load(t).start()

    def clear():
        zero_row = jnp.zeros((TILE, lanes), jnp.float32)
        zero_line = jnp.zeros((nk, lanes), jnp.float32)
        for s in range(STEPS):
            @pl.loop(0, nj)
            def _(j):
                for i in groups(0, ni, TILE):
                    for row in (TILE - 1, TILE + nk):
                        flat[s, j + 1, pl.ds((i + 1) * deep + row, TILE, stride=deep), :] = zero_row

        for side in range(2):
            def zero_j(side=side):
                for s in range(STEPS):
                    @pl.loop(0, ni)
                    def _(i):
                        field[s, (nj + 1) * side, i + 1, inside_k, :] = zero_line

            def zero_i(side=side):
                for s in range(STEPS):
                    @pl.loop(0, nj)
                    def _(j):
                        field[s, j + 1, (ni + 1) * side, inside_k, :] = zero_line

            when_edge("south", side, zero_j)
            when_edge("east", side, zero_i)

    clear()
    start_flow(1)
    wait_barrier()
    wait_face()
    for c in range(len(chunks)):
        for side in range(2):
            send_i(0, c, side, False)
    for t in range(nj):
        if t == 2:
            for c in range(len(chunks)):
                send_late(0, c)
        wait_load(t)
        pack_first(t)
        send_k(0, t)
        if t == 0:
            send_j(0)
        if t == nj - 1:
            send_far_j(0)
        if t == 0:
            for flow in flows:
                for low in (0, ni - 1):
                    load_flow_face(low, 1, *flow).start()
            start_flow(0)

    def order():
        if nj == 4:
            for word in PLAN:
                yield word[0], *map(int, word[1:])
            return
        for s in range(STEPS):
            for t in [*range(1, nj), 0]:
                yield "E", s, t
                yield "M", s, t
            if s:
                yield "D", s - 1
            for c, (t, k, size) in enumerate(chunks):
                for side in range(2):
                    yield "F", s, c, side
                if s + 1 < STEPS:
                    yield "Z", s + 1, c
                if k + size == nk:
                    yield "K", s, t
                if k + size == nk and t == 0 and s + 1 < STEPS:
                    yield "J", s + 1
            if s + 1 < STEPS:
                yield "X", s + 1
        yield "D", STEPS - 1

    def plane_at_end(low_end):
        def act():
            edge_tiles(0, 0)
            middle(0, 0)

        if n_down == 1:
            if low_end:
                act()
            return
        for piece in range(len(pieces)):
            wait_j(0, 0, piece)
        before = set(waited)
        pl.when((down == 0) if low_end else (down > 0))(act)
        if low_end:
            waited.clear()
            waited.update(before)

    def near(s):
        drain_j(s - 1)
        send_j(s)

    acts = {
        "E": edge_tiles, "M": middle, "F": face, "K": fix,
        "D": drain, "Z": send_late, "J": near, "X": send_far_j, "P": plane_at_end,
    }
    for name, *where in order():
        acts[name](*where)
    drain_j(STEPS - 1)


def per_device(counts, density, flow_j, flow_i, flow_k):
    nj, ni, nk, lanes = density.shape
    f32 = jnp.float32
    dma = pltpu.SemaphoreType.DMA
    south, down = (2 if counts[at] > 2 else 1 for at in (0, 2))
    return pl.pallas_call(
        functools.partial(kernel, counts),
        out_shape=pltpu.VMEM(density.shape, f32),
        in_specs=[pl.BlockSpec(memory_space=pl.ANY)] * 4,
        out_specs=pl.BlockSpec(memory_space=pltpu.VMEM),
        scratch_shapes=[
            pltpu.VMEM((STEPS, nj + 2, ni + 2, nk + 2 * TILE, lanes), f32),
            pltpu.VMEM((nj, ni, nk, lanes), f32),
            pltpu.VMEM((nj, ni, nk, lanes), f32),
            pltpu.VMEM((nj, ni, nk, lanes), f32),
            pltpu.VMEM((STEPS, 2, nj, ni, lanes), f32),
            pltpu.VMEM((STEPS, 2, nj, ni, lanes), f32),
            dma((nj + 1,)),
            dma((3,)),
            dma((2, 2)),
            dma((2, 2, nj + 1)),
            dma((2, down)),
            dma((2, down, nj)),
            dma((south,)),
            dma((2, south, 2)),
        ],
        compiler_params=pltpu.CompilerParams(
            collective_id=0, has_side_effects=True, vmem_limit_bytes=58 * 1024 * 1024
        ),
    )(density, flow_j, flow_i, flow_k)


def solution(mesh):
    spec = P(("ens", "south"), "east", "down", None)
    counts = tuple(mesh.shape[a] for a in ("south", "east", "down"))
    return jax.shard_map(
        functools.partial(per_device, counts),
        mesh=mesh,
        in_specs=(spec,) * 4,
        out_specs=spec,
        check_vma=False,
    )
```

```python
import functools

import jax
import jax.numpy as jnp
from jax import lax
from jax.experimental import pallas as pl
from jax.experimental.pallas import tpu as pltpu
from jax.sharding import PartitionSpec as P

STEPS = 3
TILE = 8
MESH = pl.DeviceIdType.MESH
PLAN = (
    "E01", "M01", "P1", "F000", "F010", "P0", "F001", "F011", "K00", "J1", "Z10", "Z11",
    "E02", "F020", "F021", "K01", "Z12", "F030", "F040", "F031", "K02", "Z13", "E03", "F041",
    "K03", "Z14", "M02", "M03", "X1", "A11", "B11", "D0", "F100", "F101", "F110", "F111",
    "Z20", "Z21", "E10", "K10", "M10", "J2", "C11", "F120", "F121", "K11", "Z22", "E12",
    "F130", "E13", "F140", "F131", "K12", "Z23", "F141", "K13", "Z24", "M12", "M13", "X2",
    "E21", "M21", "E22", "M22", "E23", "M23", "E20", "M20", "D1", "F200", "F201", "F210",
    "F211", "K20", "F220", "F221", "K21", "F230", "F231", "K22", "F240", "K23", "D2", "F241",
)


def divisor(total, most):
    return max(d for d in range(1, most + 1) if total % d == 0)


def groups(low, high, size):
    return [min(at, high - size) for at in range(low, high, size)]


def kernel(
    counts, density, flow_j, flow_i, flow_k, out,
    field, cj, ci, ck, pack, land,
    load_sem, flow_sem, isend, irecv, ksend, krecv, jsend, jrecv,
):
    nj, ni, nk, lanes = density.shape
    deep = nk + 2 * TILE
    n_south, n_east, n_down = counts
    south, east, down = (lax.axis_index(a) for a in ("south", "east", "down"))
    index = {"south": south, "east": east, "down": down}
    has = {
        ("south", 0): (n_south > 1, south > 0),
        ("south", 1): (n_south > 1, south < n_south - 1),
        ("east", 0): (n_east > 1, east > 0),
        ("east", 1): (n_east > 1, east < n_east - 1),
        ("down", 0): (n_down > 1, down > 0),
        ("down", 1): (n_down > 1, down < n_down - 1),
    }
    inside_k = pl.ds(TILE, nk)
    wide = divisor(ni - 2, 10)
    tall = divisor(ni - 2, 30)
    pieces = [(0, ni // 2), (ni // 2, ni)]
    half = max(TILE, nk * 3 // 4 // TILE * TILE)
    chunks = [(0, 0, half), (0, half, nk - half)] + [(t, 0, nk) for t in range(1, nj)]

    def slot(axis, side):
        return side if counts[("south", "east", "down").index(axis)] > 2 else 0

    def neighbour(axis, side):
        return {axis: index[axis] + (1 if side else -1)}

    def when_has(axis, side, act):
        static, dynamic = has[axis, side]
        if static:
            pl.when(dynamic)(act)

    def when_edge(axis, side, act):
        static, dynamic = has[axis, side]
        if static:
            pl.when(jnp.logical_not(dynamic))(act)
        else:
            act()

    first = jnp.where(south == 0, 1, 0) if n_south > 1 else 0

    def plane(t):
        return first * (nj - 1 - t) + (1 - first) * t

    between = pl.ds(1, ni - 2)

    def load(t):
        return pltpu.make_async_copy(
            density.at[plane(t), between],
            field.at[0, plane(t) + 1, pl.ds(2, ni - 2), inside_k],
            load_sem.at[t],
        )

    def load_face(low, rows, high):
        return pltpu.make_async_copy(
            density.at[:, pl.ds(low, rows)],
            field.at[0, pl.ds(1, nj), pl.ds(high, rows), inside_k],
            load_sem.at[nj],
        )

    flows = ((flow_j, cj), (flow_i, ci), (flow_k, ck))

    def flow_slot(t):
        return flow_sem.at[t] if t < 2 else load_sem.at[t - 2]

    def load_flow(t, source, target):
        return pltpu.make_async_copy(
            source.at[plane(t), between], target.at[plane(t), between], flow_slot(t)
        )

    def load_flow_face(low, rows, source, target):
        return pltpu.make_async_copy(
            source.at[:, pl.ds(low, rows)], target.at[:, pl.ds(low, rows)], flow_sem.at[2]
        )

    def copy_i(s, side, c):
        t, k, size = chunks[c]
        j, part = plane(t), pl.ds(TILE + k, size)
        return pltpu.make_async_remote_copy(
            src_ref=field.at[s, j + 1, ni if side else 1, part],
            dst_ref=field.at[s, j + 1, 0 if side else ni + 1, part],
            send_sem=isend.at[s % 2, side],
            recv_sem=irecv.at[s % 2, 1 - side, c],
            device_id=neighbour("east", side),
            device_id_type=MESH,
        )

    def copy_k(s, side, j):
        return pltpu.make_async_remote_copy(
            src_ref=pack.at[s, side, j],
            dst_ref=land.at[s, 1 - side, j],
            send_sem=ksend.at[s % 2, slot("down", side)],
            recv_sem=krecv.at[s % 2, slot("down", 1 - side), j],
            device_id=neighbour("down", side),
            device_id_type=MESH,
        )

    def copy_j(s, side, piece):
        low, high = pieces[piece]
        rows = pl.ds(low + 1, high - low)
        return pltpu.make_async_remote_copy(
            src_ref=field.at[s, nj if side else 1, rows, inside_k],
            dst_ref=field.at[s, 0 if side else nj + 1, rows, inside_k],
            send_sem=jsend.at[slot("south", side)],
            recv_sem=jrecv.at[s % 2, slot("south", 1 - side), piece],
            device_id=neighbour("south", side),
            device_id_type=MESH,
        )

    def send_i(s, c, side, late):
        static, dynamic = has["east", side]
        if static and n_south > 1:
            pl.when(dynamic & ((south > 0) if late else (south == 0)))(copy_i(s, side, c).start)
        elif static and not late:
            pl.when(dynamic)(copy_i(s, side, c).start)

    def send_late(s, c):
        for side in range(2):
            send_i(s, c, side, True)

    def send_k(s, t):
        for side in range(2):
            when_has("down", side, lambda side=side: copy_k(s, side, plane(t)).start())

    def start_j(s, side):
        for piece in range(len(pieces)):
            copy_j(s, side, piece).start()

    def send_j(s):
        if n_south > 1:
            pl.when(south == 0)(lambda: start_j(s, 1))
            pl.when(south > 0)(lambda: start_j(s, 0))

    def send_far_j(s):
        if n_south > 2:
            pl.when((south > 0) & (south < n_south - 1))(lambda: start_j(s, 1))

    waited = set()

    def wait_j(s, t, piece):
        if (s, t, piece) in waited:
            return
        waited.add((s, t, piece))
        if n_south > 1 and t == 0:
            pl.when(south == 0)(lambda: copy_j(s, 0, piece).wait_recv())
            pl.when(south > 0)(lambda: copy_j(s, 1, piece).wait_recv())
        if n_south > 2 and t == nj - 1:
            pl.when((south > 0) & (south < n_south - 1))(
                lambda: copy_j(s, 0, piece).wait_recv()
            )

    def wait_i(s, c, side):
        when_has("east", side, lambda: copy_i(s, 1 - side, c).wait_recv())

    def rows(s, j, i, count, k=0, size=nk):
        def at(dj, di, dk):
            return field[s, j + 1 + dj, i + 1 + di, pl.ds(TILE + k + dk, size), :]

        line = [at(0, r - 1, 0) for r in range(count + 2)]
        for r in range(count):
            cell = (j, i + r, pl.ds(k, size))
            lower = [at(-1, r, 0), line[r], at(0, r, -1)]
            upper = [at(1, r, 0), line[r + 2], at(0, r, 1)]
            gain = [c[cell] for c in (cj, ci, ck)]
            if s == 0:
                gain = [0.05 - g for g in gain]
                for c, g in zip((cj, ci, ck), gain):
                    c[cell] = g
            drift = [g * (u - l) for g, u, l in zip(gain, upper, lower)]
            value = (0.7 * line[r + 1] + 0.1 * (lower[0] + lower[1] + lower[2])) + (
                drift[0] + drift[1] + drift[2]
            )
            if s + 1 < STEPS:
                field[s + 1, j + 1, i + 1 + r, pl.ds(TILE + k, size), :] = value
            else:
                out[cell] = value

    flat = field.reshape(STEPS, nj + 2, (ni + 2) * deep, lanes)
    flat_gain = ck.reshape(nj, ni * nk, lanes)
    flat_out = out.reshape(nj, ni * nk, lanes)

    def edge_field(s, j, i, size, side):
        row = (i + 1) * deep + TILE + (nk - 1) * side
        return flat.at[s, j + 1, pl.ds(row, size, stride=deep), :]

    def edge(ref, j, i, size, side):
        return ref.at[j, pl.ds(i * nk + (nk - 1) * side, size, stride=nk), :]

    def start_flow(t):
        for flow in flows:
            load_flow(t, *flow).start()

    def wait_flow(t):
        pltpu.make_async_copy(
            flow_j.at[pl.ds(0, 3), between], cj.at[pl.ds(0, 3), between], flow_slot(t)
        ).wait()
        for later in [2] if t == 1 else range(3, nj) if t == 0 else []:
            start_flow(later)

    def ready(s, t):
        if s == 0 and (t, "flow") not in waited:
            waited.add((t, "flow"))
            wait_flow(t)
        for piece in range(len(pieces)):
            wait_j(s, t, piece)

    def edge_tiles(s, t):
        ready(s, t)

        @pl.loop(0, (ni - 2) // tall)
        def _(b):
            for k in sorted({0, nk - TILE}):
                rows(s, plane(t), 1 + b * tall, tall, k, TILE)

    def middle(s, t):
        ready(s, t)
        if nk > 2 * TILE:
            @pl.loop(0, (ni - 2) // wide)
            def _(b):
                rows(s, plane(t), 1 + b * wide, wide, TILE, nk - 2 * TILE)

    def wait_k(s, t, side):
        if (s, t, side, "k") in waited:
            return
        waited.add((s, t, side, "k"))
        j = plane(t)

        def corner():
            copy_k(s, 1 - side, j).wait_recv()
            row = TILE + nk if side else TILE - 1
            for i in (0, ni - 1):
                field[s, j + 1, i + 1, pl.ds(row, 1), :] = land[s, side, j, pl.ds(i, 1), :]

        when_has("down", side, corner)

    def face(s, c, side):
        t, k, size = chunks[c]
        for piece in range(len(pieces)):
            wait_j(s, t, piece)
        if k == 0:
            wait_k(s, t, 0)
        if k + size == nk:
            wait_k(s, t, 1)
        if s == 0 and "faces" not in waited:
            waited.add("faces")
            wait_flow_face()
        wait_i(s, c, side)
        rows(s, plane(t), (ni - 1) * side, 1, k, size)
        if s + 1 < STEPS:
            send_i(s + 1, c, side, False)

    def fix(s, t):
        j = plane(t)
        for side in range(2):
            def act(side=side):
                parts = []
                for i in groups(1, ni - 1, TILE):
                    gain = edge(flat_gain, j, i, TILE, side)[...]
                    gain = gain if side else 0.1 - gain
                    if s + 1 < STEPS:
                        target = edge_field(s + 1, j, i, TILE, side)
                    else:
                        target = edge(flat_out, j, i, TILE, side)
                    value = target[...] + gain * land[s, side, j, pl.ds(i, TILE), :]
                    parts.append((i, target, value))
                for i, target, value in parts:
                    target[...] = value
                    if s + 1 < STEPS:
                        pack[s + 1, side, j, pl.ds(i, TILE), :] = value
                if s + 1 < STEPS:
                    k = TILE + (nk - 1) * side
                    for i in (0, ni - 1):
                        pack[s + 1, side, j, pl.ds(i, 1), :] = field[
                            s + 1, j + 1, i + 1, pl.ds(k, 1), :
                        ]
            when_has("down", side, act)
        if s + 1 < STEPS:
            send_k(s + 1, t)

    def drain_i(s):
        for side in range(2):
            def sent(side=side):
                pltpu.make_async_remote_copy(
                    src_ref=field.at[s, pl.ds(1, nj), ni if side else 1, inside_k],
                    dst_ref=field.at[s, pl.ds(1, nj), 0 if side else ni + 1, inside_k],
                    send_sem=isend.at[s % 2, side],
                    recv_sem=irecv.at[s % 2, 1 - side, 0],
                    device_id=neighbour("east", side),
                    device_id_type=MESH,
                ).wait_send()
            when_has("east", side, sent)

    def drain_k(s):
        for side in range(2):
            def sent(side=side):
                pltpu.make_async_remote_copy(
                    src_ref=pack.at[s, side],
                    dst_ref=land.at[s, 1 - side],
                    send_sem=ksend.at[s % 2, slot("down", side)],
                    recv_sem=krecv.at[s % 2, slot("down", 1 - side), 0],
                    device_id=neighbour("down", side),
                    device_id_type=MESH,
                ).wait_send()
            when_has("down", side, sent)

    def drain_j(s):
        for side in range(2):
            def sent(side=side):
                rows = pl.ds(1, ni)
                pltpu.make_async_remote_copy(
                    src_ref=field.at[s, nj if side else 1, rows, inside_k],
                    dst_ref=field.at[s, 0 if side else nj + 1, rows, inside_k],
                    send_sem=jsend.at[slot("south", side)],
                    recv_sem=jrecv.at[s % 2, slot("south", 1 - side), 0],
                    device_id=neighbour("south", side),
                    device_id_type=MESH,
                ).wait_send()
            when_has("south", side, sent)

    def drain(s):
        drain_i(s)
        drain_k(s)

    def wait_load(t):
        load(t).wait()

    def pack_first(t):
        for side in range(2):
            def act(side=side):
                for i in groups(0, ni, TILE):
                    pack[0, side, plane(t), pl.ds(i, TILE), :] = edge_field(
                        0, plane(t), i, TILE, side
                    )[...]
            when_has("down", side, act)

    def wait_barrier():
        pl.semaphore_wait(barrier, sum(jnp.where(d, 1, 0) for s, d in has.values() if s))

    def wait_face():
        load_face(0, 2, 1).wait()

    def wait_flow_face():
        load_flow_face(0, 6, flow_j, cj).wait()

    barrier = pltpu.get_barrier_semaphore()
    for axis, side in has:
        def greet(axis=axis, side=side):
            pl.semaphore_signal(
                barrier, inc=1, device_id=neighbour(axis, side), device_id_type=MESH
            )
        when_has(axis, side, greet)

    for low in (0, ni - 1):
        load_face(low, 1, low + 1).start()
    for t in range(nj):
        load(t).start()

    def clear():
        zero_row = jnp.zeros((TILE, lanes), jnp.float32)
        zero_line = jnp.zeros((nk, lanes), jnp.float32)
        for s in range(STEPS):
            @pl.loop(0, nj)
            def _(j):
                for i in groups(0, ni, TILE):
                    for row in (TILE - 1, TILE + nk):
                        flat[s, j + 1, pl.ds((i + 1) * deep + row, TILE, stride=deep), :] = zero_row

        for side in range(2):
            def zero_j(side=side):
                for s in range(STEPS):
                    @pl.loop(0, ni)
                    def _(i):
                        field[s, (nj + 1) * side, i + 1, inside_k, :] = zero_line

            def zero_i(side=side):
                for s in range(STEPS):
                    @pl.loop(0, nj)
                    def _(j):
                        field[s, j + 1, (ni + 1) * side, inside_k, :] = zero_line

            when_edge("south", side, zero_j)
            when_edge("east", side, zero_i)

    clear()
    start_flow(1)
    wait_barrier()
    wait_face()
    for c in range(len(chunks)):
        for side in range(2):
            send_i(0, c, side, False)
    for t in range(nj):
        if t == 2:
            for c in range(len(chunks)):
                send_late(0, c)
        wait_load(t)
        pack_first(t)
        send_k(0, t)
        if t == 0:
            send_j(0)
        if t == nj - 1:
            send_far_j(0)
        if t == 0:
            for flow in flows:
                for low in (0, ni - 1):
                    load_flow_face(low, 1, *flow).start()
            start_flow(0)

    def order():
        if nj == 4:
            for word in PLAN:
                yield word[0], *map(int, word[1:])
            return
        for s in range(STEPS):
            for t in [*range(1, nj), 0]:
                yield "E", s, t
                yield "M", s, t
            if s:
                yield "D", s - 1
            for c, (t, k, size) in enumerate(chunks):
                for side in range(2):
                    yield "F", s, c, side
                if s + 1 < STEPS:
                    yield "Z", s + 1, c
                if k + size == nk:
                    yield "K", s, t
                if k + size == nk and t == 0 and s + 1 < STEPS:
                    yield "J", s + 1
            if s + 1 < STEPS:
                yield "X", s + 1
        yield "D", STEPS - 1

    def when_end(low_end, act):
        if n_down > 1:
            pl.when((down == 0) if low_end else (down > 0))(act)
        elif low_end:
            act()

    def whole(s, t):
        edge_tiles(s, t)
        middle(s, t)

    def first_plane(low_end):
        for piece in range(len(pieces)):
            wait_j(0, 0, piece)
        before = set(waited)
        when_end(low_end, lambda: whole(0, 0))
        if low_end:
            waited.clear()
            waited.update(before)

    def low_plane(s, t):
        when_end(True, lambda: whole(s, t))

    def high_edge(s, t):
        when_end(False, lambda: edge_tiles(s, t))

    def high_middle(s, t):
        when_end(False, lambda: middle(s, t))

    def near(s):
        drain_j(s - 1)
        send_j(s)

    acts = {
        "E": edge_tiles, "M": middle, "F": face, "K": fix,
        "D": drain, "Z": send_late, "J": near, "X": send_far_j,
        "P": first_plane, "A": low_plane, "B": high_edge, "C": high_middle,
    }
    for name, *where in order():
        acts[name](*where)
    drain_j(STEPS - 1)


def store(end, out, sem):
    for j in range(out.shape[0]):
        pltpu.make_async_copy(end.at[j], out.at[j], sem).start()
    pltpu.make_async_copy(end, out, sem).wait()


def per_device(counts, density, flow_j, flow_i, flow_k):
    nj, ni, nk, lanes = density.shape
    f32 = jnp.float32
    dma = pltpu.SemaphoreType.DMA
    south, down = (2 if counts[at] > 2 else 1 for at in (0, 2))
    end = pl.pallas_call(
        functools.partial(kernel, counts),
        out_shape=pltpu.VMEM(density.shape, f32),
        in_specs=[pl.BlockSpec(memory_space=pl.ANY)] * 4,
        out_specs=pl.BlockSpec(memory_space=pltpu.VMEM),
        scratch_shapes=[
            pltpu.VMEM((STEPS, nj + 2, ni + 2, nk + 2 * TILE, lanes), f32),
            pltpu.VMEM((nj, ni, nk, lanes), f32),
            pltpu.VMEM((nj, ni, nk, lanes), f32),
            pltpu.VMEM((nj, ni, nk, lanes), f32),
            pltpu.VMEM((STEPS, 2, nj, ni, lanes), f32),
            pltpu.VMEM((STEPS, 2, nj, ni, lanes), f32),
            dma((nj + 1,)),
            dma((3,)),
            dma((2, 2)),
            dma((2, 2, nj + 1)),
            dma((2, down)),
            dma((2, down, nj)),
            dma((south,)),
            dma((2, south, 2)),
        ],
        compiler_params=pltpu.CompilerParams(
            collective_id=0, has_side_effects=True, vmem_limit_bytes=58 * 1024 * 1024
        ),
    )(density, flow_j, flow_i, flow_k)
    return pl.pallas_call(
        store,
        out_shape=jax.ShapeDtypeStruct(density.shape, f32),
        in_specs=[pl.BlockSpec(memory_space=pltpu.VMEM)],
        out_specs=pl.BlockSpec(memory_space=pl.ANY),
        scratch_shapes=[dma],
        compiler_params=pltpu.CompilerParams(vmem_limit_bytes=1024 * 1024),
    )(end)


def solution(mesh):
    spec = P(("ens", "south"), "east", "down", None)
    counts = tuple(mesh.shape[a] for a in ("south", "east", "down"))
    return jax.shard_map(
        functools.partial(per_device, counts),
        mesh=mesh,
        in_specs=(spec,) * 4,
        out_specs=spec,
        check_vma=False,
    )
```
